32 devices in a mesh: state: 2 (over x), bond: 16 (over z, y, core).
Axes of the slice: x: 2, y: 2, z: 4, core: 2. Of those that a mesh axis runs over, the one named last changes fastest.
Arguments:
- intersect_left: bfloat16 [2, 2048, 2048], P('state', 'bond'), may hold values from -0.125 to 0.125
- stored_block: bfloat16 [2, 4, 2048, 2048], P('state', None, 'bond'), may hold values from -6 to 6
- stored_site: bfloat16 [2, 2, 2048, 2048], P('state', None, 'bond'), may hold values from -6 to 6
- current_site: bfloat16 [2048, 2, 2048], P('bond', None, 'state'), may hold values from -0.09375 to 0.09375
- current_block: bfloat16 [4, 2048, 2048], P(None, 'bond', 'state'), may hold values from -6 to 6
- penalty_weight: float32 [2], replicated, may hold values from 0.5 to 4
Outputs:
- penalized: float32 [4, 2048, 2048], P(None, 'bond', 'state')
- intersect_next: bfloat16 [2, 2048, 2048], P('state', 'bond')
The draws below stay inside these ranges and needn't reach their ends.
All inputs are finite; a program needn't handle non-finite values.
Results may differ from the reference program's by a relative error of at most 0.0055.
Values may be sent and summed in bfloat16 or wider, within the bound.
A program may use at most 64 MiB of HBM per device.

```python
import math
import jax
import jax.numpy as jnp

D = 2048
PHYS = 2
Q = 4
STATES = 2


def level_of(rng, dims, pieces, least, high):
    def one(axis_at, shards_of):
        draws = jax.random.uniform(jax.random.fold_in(jax.random.fold_in(rng, 6), axis_at), (shards_of,), jnp.float32, least / len(pieces), high / len(pieces))
        return jnp.repeat(jnp.exp(draws), dims[axis_at] // shards_of).reshape((-1,) + (1,) * (len(dims) - axis_at - 1))

    factor_of = one(*pieces[0])
    for cut in pieces[1:]:
        factor_of = factor_of * one(*cut)
    return factor_of


def normal_values(key, dims, scale, limit, split=(), kind=jnp.bfloat16):
    result = scale * jax.random.normal(key, dims, jnp.float32)
    if split:
        result = result * level_of(key, dims, split, -0.22, 0.18)
    return jnp.clip(result, -limit, limit).astype(kind)


def setup_inputs(seed: int = 0) -> dict:
    seeds = jax.random.split(jax.random.key(seed), 7)
    return {
        "intersect_left": normal_values(seeds[0], (STATES, D, D), D ** -0.5, 0.125, ((0, 2), (1, 16))),
        "stored_block": normal_values(seeds[1], (STATES, Q, D, D), 1.0, 6.0, ((0, 2), (2, 16))),
        "stored_site": normal_values(seeds[2], (STATES, PHYS, D, D), 1.0, 6.0, ((0, 2), (2, 16))),
        "current_site": normal_values(seeds[3], (D, PHYS, D), (PHYS * D) ** -0.5, 0.09375, ((0, 16), (2, 2))),
        "current_block": normal_values(seeds[4], (Q, D, D), 1.0, 6.0, ((1, 16), (2, 2))),
        "penalty_weight": jnp.clip(jnp.exp(jax.random.uniform(seeds[5], (STATES,), jnp.float32, math.log(0.5), math.log(4.0))), 0.5, 4.0),
    }


def reference(intersect_left, stored_block, stored_site, current_site, current_block, penalty_weight):
    block_wide = current_block.astype(jnp.float32)
    site_wide = current_site.astype(jnp.float32)
    penalized = block_wide
    grown_list = []
    for index in range(STATES):
        env_turned = intersect_left[index].T
        projected = jnp.dot(stored_block[index].reshape(Q * D, D), env_turned, preferred_element_type=jnp.float32).reshape(Q, D, D)
        intersect = jnp.sum(projected * block_wide) / (PHYS * D)
        penalized = penalized + (penalty_weight[index] * intersect) * projected
        moved = jnp.dot(stored_site[index].reshape(PHYS * D, D), env_turned, preferred_element_type=jnp.float32).astype(jnp.bfloat16)
        moved = moved.reshape(PHYS, D, D).astype(jnp.float32)
        grown = jnp.einsum("asf,sea->fe", site_wide, moved).astype(jnp.bfloat16)
        grown_list.append(grown)
    return penalized, jnp.stack(grown_list)
```

```python
import functools

import jax
import jax.numpy as jnp
from jax import lax
from jax.experimental import pallas as pl
from jax.experimental.pallas import tpu as pltpu
from jax.sharding import PartitionSpec as P

MESH = pl.DeviceIdType.MESH
CORES = 2
TILE = 256


def kernel(
    states, bonds, rows_y,
    env_hbm, block_hbm, site_hbm, grow_hbm, current_hbm, weight_ref,
    pen_hbm, next_hbm,
    ebuf, abuf, stored, cbuf, psend, precv, mbuf, acc, pen, nsend, nrecv, iall,
    local_sem, out_sem, e_send, e_recv, a_send, a_recv, p_send, p_recv, m_send, m_recv,
    i_send, i_recv, n_send, n_recv, c_send, c_recv, line,
):
    nc, ny = CORES, rows_y
    nz = bonds // (nc * ny)
    rows, width = ebuf.shape[1:]
    pairs = block_hbm.shape[0]
    phys = site_hbm.shape[0]
    w = block_hbm.shape[1]
    per_group = TILE // rows
    per_row = ny * nc * rows // TILE
    groups = width // TILE
    gpp = groups // states
    fwidth = abuf.shape[2] // phys
    nfb = fwidth // w
    count = states * bonds

    k = lax.axis_index("state")
    me = lax.axis_index("bond")
    c = lax.rem(me, nc)
    y = lax.rem(lax.div(me, nc), ny)
    z = lax.div(me, nc * ny)
    flat = k * bonds + me

    def slot(zz, yy, cc):
        return (zz * ny + yy) * nc + cc

    e_load = pltpu.make_async_copy(env_hbm, ebuf.at[me], local_sem.at[0])
    a_load = pltpu.make_async_copy(grow_hbm, abuf.at[me], local_sem.at[1])
    e_load.start()
    c_loads = [
        pltpu.make_async_copy(
            current_hbm.at[:, :, pl.ds(g * TILE, TILE)], cbuf.at[k * gpp + g], local_sem.at[3]
        )
        for g in range(gpp)
    ]
    for copy in c_loads:
        copy.start()
    loads = []
    for q in range(pairs):
        loads.append(pltpu.make_async_copy(block_hbm.at[q], stored.at[pl.ds(q * w, w)], local_sem.at[2]))
    for s in range(phys):
        loads.append(
            pltpu.make_async_copy(site_hbm.at[s], stored.at[pl.ds((pairs + s) * w, w)], local_sem.at[2])
        )
    for copy in loads:
        copy.start()
    a_load.start()

    barrier = pltpu.get_barrier_semaphore()

    @pl.loop(1, count)
    def _(r):
        peer = lax.rem(flat + r, count)
        pl.semaphore_signal(
            barrier, inc=1, device_id=(lax.div(peer, bonds), lax.rem(peer, bonds)), device_id_type=MESH
        )

    pl.semaphore_wait(barrier, count - 1)

    env = (ebuf, e_send, e_recv)
    site = (abuf, a_send, a_recv)

    def copy_of(what, blk, dest):
        buf, ss, rs = what
        return pltpu.make_async_remote_copy(
            src_ref=buf.at[blk], dst_ref=buf.at[blk], send_sem=ss, recv_sem=rs.at[blk],
            device_id=(k, dest), device_id_type=MESH,
        )

    def act(what, blk, dest, drain):
        copy = copy_of(what, blk, dest)
        if drain:
            copy.wait_send()
        else:
            copy.start()

    def arrive(what, blk):
        copy_of(what, blk, me).wait_recv()

    def spread(what, blk, drain):
        @pl.when(y > 0)
        def _():
            act(what, blk, slot(z, y - 1, c), drain)

        @pl.when(y < ny - 1)
        def _():
            act(what, blk, slot(z, y + 1, c), drain)

        act(what, blk, slot(z, y, 1 - c), drain)

    def column(what, i, drain=False):
        if i == 0:
            blk = slot(z, y, c)

            @pl.when(z > 0)
            def _():
                act(what, blk, slot(z - 1, y, c), drain)

            @pl.when(z < nz - 1)
            def _():
                act(what, blk, slot(z + 1, y, c), drain)

            spread(what, blk, drain)
            return
        for sign in (1, -1):
            zz = z - sign * i
            onward = z + sign

            @pl.when(jnp.logical_and(zz >= 0, zz < nz))
            def _():
                blk = slot(zz, y, c)
                if not drain:
                    arrive(what, blk)

                @pl.when(jnp.logical_and(onward >= 0, onward < nz))
                def _():
                    act(what, blk, slot(onward, y, c), drain)

                spread(what, blk, drain)

    def turn(j):
        least = jnp.minimum(z, nz - 1 - z)
        near = (j + 1) // 2
        inner = z - near if j % 2 else z + near
        far = j - least
        outer = jnp.where(z <= nz - 1 - z, z + far, z - far)
        return jnp.where(j <= 2 * least, inner, outer)

    def across(what, j, drain=False):
        zz = turn(j)
        for u in range(1, ny):
            for sign in (1, -1):
                yy = y - sign * u
                onward = y + sign

                @pl.when(jnp.logical_and(yy >= 0, yy < ny))
                def _():
                    blk = slot(zz, yy, c)
                    if not drain:
                        arrive(what, blk)

                    @pl.when(jnp.logical_and(onward >= 0, onward < ny))
                    def _():
                        act(what, blk, slot(z, onward, c), drain)

                    act(what, blk, slot(z, y, 1 - c), drain)

    def sibling(what, j):
        zz = turn(j)
        for yy in range(ny):
            arrive(what, slot(zz, yy, 1 - c))

    def p_copy(g, peer):
        return pltpu.make_async_remote_copy(
            src_ref=psend.at[g], dst_ref=precv.at[k, lax.rem(g, gpp)], send_sem=p_send,
            recv_sem=p_recv.at[k], device_id=(peer, me), device_id_type=MESH,
        )

    def m_copy(g, peer):
        return pltpu.make_async_remote_copy(
            src_ref=mbuf.at[g, :, k], dst_ref=mbuf.at[g, :, k], send_sem=m_send,
            recv_sem=m_recv.at[k], device_id=(peer, me), device_id_type=MESH,
        )

    def c_copy(zz, peer):
        part = pl.ds(zz * per_row, per_row)
        return pltpu.make_async_remote_copy(
            src_ref=cbuf.at[part], dst_ref=cbuf.at[part], send_sem=c_send, recv_sem=c_recv.at[zz],
            device_id=(peer, me), device_id_type=MESH,
        )

    def share(drain=False):
        for j in range(nz):
            zz = turn(j)

            @pl.when(lax.div(zz * per_row, gpp) == k)
            def _():
                for other in range(1, states):
                    copy = c_copy(zz, lax.rem(k + other, states))
                    if drain:
                        copy.wait_send()
                    else:
                        copy.start()

    def project(j):
        zz = turn(j)

        @pl.when(lax.div(zz * per_row, gpp) != k)
        def _():
            c_copy(zz, k).wait_recv()

        @pl.loop(0, per_row)
        def _(r):
            g = zz * per_row + r
            left = ebuf[pl.ds(g * per_group, per_group)].reshape(TILE, width)
            prod = lax.dot_general(
                stored[...], left, (((1,), (1,)), ((), ())), preferred_element_type=jnp.float32
            )
            mbuf[g, :, k] = prod[pairs * w :].astype(jnp.bfloat16).reshape(phys, w, TILE)
            whole = prod[: pairs * w]
            here = cbuf[g].reshape(pairs * w, TILE).astype(jnp.float32)
            line[...] += jnp.sum((whole * here).reshape(pairs * w // 8, 8, TILE), axis=0)
            part = whole.astype(jnp.bfloat16)
            psend[g] = part
            owner = lax.div(g, gpp)

            @pl.when(owner == k)
            def _():
                precv[k, lax.rem(g, gpp)] = part

            for other in range(1, states):
                peer = lax.rem(k + other, states)

                m_copy(g, peer).start()

                @pl.when(owner == peer)
                def _():
                    p_copy(g, peer).start()

    def grow(j):
        zz = turn(j)

        @pl.loop(0, per_row)
        def _(r):
            g = zz * per_row + r
            right = abuf[pl.ds(g * per_group, per_group)].reshape(TILE, phys * fwidth)
            total = jnp.zeros((states * w, fwidth), jnp.float32)
            for s in range(phys):
                total = total + jnp.dot(
                    mbuf[g, s].reshape(states * w, TILE),
                    right[:, s * fwidth : (s + 1) * fwidth],
                    preferred_element_type=jnp.float32,
                )
            acc[...] += total

    def overlap():
        short = jnp.sum(line[...], axis=0, keepdims=True)
        total = short[:, :128]
        for at in range(128, TILE, 128):
            total = total + short[:, at : at + 128]
        iall[flat] = total

    def i_copy(peer):
        return pltpu.make_async_remote_copy(
            src_ref=iall.at[flat], dst_ref=iall.at[flat], send_sem=i_send, recv_sem=i_recv,
            device_id=(lax.div(peer, bonds), lax.rem(peer, bonds)), device_id_type=MESH,
        )

    def tell():
        @pl.loop(1, count)
        def _(r):
            i_copy(lax.rem(flat + r, count)).start()

    pen_copies = [
        pltpu.make_async_copy(pen.at[g], pen_hbm.at[:, :, pl.ds(g * TILE, TILE)], out_sem.at[0])
        for g in range(gpp)
    ]

    def penalize():
        rest = iall.at[pl.ds(0, count - 1)]
        pltpu.make_async_remote_copy(
            src_ref=rest, dst_ref=rest, send_sem=i_send, recv_sem=i_recv,
            device_id=(k, me), device_id_type=MESH,
        ).wait_recv()
        for other in range(1, states):
            peer = lax.rem(k + other, states)
            pltpu.make_async_remote_copy(
                src_ref=precv.at[peer], dst_ref=precv.at[peer], send_sem=p_send,
                recv_sem=p_recv.at[peer], device_id=(peer, me), device_id_type=MESH,
            ).wait_recv()
        scale = 1.0 / (phys * width)
        factors = [
            weight_ref[kk] * (jnp.sum(iall[kk * bonds : (kk + 1) * bonds]) * scale)
            for kk in range(states)
        ]
        for g in range(gpp):
            value = cbuf[k * gpp + g].reshape(pairs * w, TILE).astype(jnp.float32)
            for kk in range(states):
                value = value + factors[kk] * precv[kk, g].astype(jnp.float32)
            pen[g] = value.reshape(pairs, w, TILE)
            pen_copies[g].start()

    acc[...] = jnp.zeros_like(acc)
    line[...] = jnp.zeros_like(line)
    e_load.wait()
    for i in range(2 * nz):
        if i < nz:
            column(env, i)
        if i == 0:
            for copy in c_loads:
                copy.wait()
            share()
        if i >= nz - 1 and i - (nz - 1) < nz:
            if i == nz - 1:
                a_load.wait()
            column(site, i - (nz - 1))
        if 1 <= i <= nz:
            across(env, i - 1)
            sibling(env, i - 1)
            if i == 1:
                for copy in loads:
                    copy.wait()
            project(i - 1)
            if i == nz:
                overlap()
                tell()
        if i >= nz:
            across(site, i - nz)
            sibling(site, i - nz)
            if i == nz:
                for other in range(1, states):
                    peer = lax.rem(k + other, states)
                    mine = mbuf.at[:, :, peer]
                    pltpu.make_async_remote_copy(
                        src_ref=mine, dst_ref=mine, send_sem=m_send, recv_sem=m_recv.at[peer],
                        device_id=(peer, me), device_id_type=MESH,
                    ).wait_recv()
            grow(i - nz)
            if i == min(nz + 1, 2 * nz - 1):
                penalize()

    def n_copy(kk, fb):
        return pltpu.make_async_remote_copy(
            src_ref=nsend.at[kk, fb], dst_ref=nrecv.at[me], send_sem=n_send, recv_sem=n_recv,
            device_id=(kk, k * nfb + fb), device_id_type=MESH,
        )

    def is_me(kk, fb):
        return jnp.logical_and(k == kk, me == k * nfb + fb)

    for kk in range(states):
        for fb in range(nfb):
            part = acc[kk * w : (kk + 1) * w, fb * w : (fb + 1) * w].T.astype(jnp.bfloat16)
            nsend[kk, fb] = part

            @pl.when(is_me(kk, fb))
            def _():
                nrecv[me] = part

            @pl.when(jnp.logical_not(is_me(kk, fb)))
            def _():
                n_copy(kk, fb).start()

    inside = lax.div(me, nfb) == k

    def all_of(number):
        rest = nrecv.at[pl.ds(0, number)]
        return pltpu.make_async_remote_copy(
            src_ref=rest, dst_ref=rest, send_sem=n_send, recv_sem=n_recv,
            device_id=(k, me), device_id_type=MESH,
        )

    for i in range(nz):
        for what in (env, site):
            column(what, i, drain=True)
            across(what, i, drain=True)

    share(drain=True)

    @pl.loop(0, groups)
    def _(g):
        for other in range(1, states):
            peer = lax.rem(k + other, states)

            @pl.when(lax.div(g, gpp) == peer)
            def _():
                p_copy(g, peer).wait_send()

            m_copy(g, peer).wait_send()

    @pl.loop(1, count)
    def _(r):
        i_copy(lax.rem(flat + r, count)).wait_send()

    for copy in pen_copies:
        copy.wait()
    for kk in range(states):
        for fb in range(nfb):
            @pl.when(jnp.logical_not(is_me(kk, fb)))
            def _():
                n_copy(kk, fb).wait_send()

    @pl.when(inside)
    def _():
        all_of(bonds - 1).wait_recv()

    @pl.when(jnp.logical_not(inside))
    def _():
        all_of(bonds).wait_recv()

    store = pltpu.make_async_copy(nrecv, next_hbm, out_sem.at[1])
    store.start()
    store.wait()


def shards(states, bonds, intersect_left, stored_block, stored_site, current_site, current_block, penalty_weight):
    rows, width = intersect_left.shape[1:]
    pairs, w = stored_block.shape[1:3]
    phys = stored_site.shape[1]
    fwidth = current_site.shape[2]
    groups = width // TILE
    gpp = groups // states
    rows_y = 1
    while 4 * rows_y * rows_y <= bonds // CORES:
        rows_y *= 2
    bf, f32 = jnp.bfloat16, jnp.float32
    anywhere = pl.BlockSpec(memory_space=pl.ANY)
    dma = pltpu.SemaphoreType.DMA
    penalized, grown = pl.pallas_call(
        functools.partial(kernel, states, bonds, rows_y),
        out_shape=(
            jax.ShapeDtypeStruct(current_block.shape, f32),
            jax.ShapeDtypeStruct((bonds, w, w), bf),
        ),
        in_specs=[anywhere] * 5 + [pl.BlockSpec(memory_space=pltpu.SMEM)],
        out_specs=(anywhere, anywhere),
        scratch_shapes=[
            pltpu.VMEM((bonds, rows, width), bf),
            pltpu.VMEM((bonds, rows, phys * fwidth), bf),
            pltpu.VMEM(((pairs + phys) * w, width), bf),
            pltpu.VMEM((groups, pairs, w, TILE), bf),
            pltpu.VMEM((groups, pairs * w, TILE), bf),
            pltpu.VMEM((states, gpp, pairs * w, TILE), bf),
            pltpu.VMEM((groups, phys, states, w, TILE), bf),
            pltpu.VMEM((states * w, fwidth), f32),
            pltpu.VMEM((gpp, pairs, w, TILE), f32),
            pltpu.VMEM((states, fwidth // w, w, w), bf),
            pltpu.VMEM((bonds, w, w), bf),
            pltpu.VMEM((states * bonds, 1, 128), f32),
            dma((4,)), dma((2,)),
            dma, dma((bonds,)), dma, dma((bonds,)),
            dma, dma((states,)), dma, dma((states,)),
            dma, dma, dma, dma,
            dma, dma((bonds,)),
            pltpu.VMEM((8, TILE), f32),
        ],
        compiler_params=pltpu.CompilerParams(
            collective_id=0, has_side_effects=True, vmem_limit_bytes=60 * 1024 * 1024
        ),
    )(
        intersect_left[0], stored_block[0], stored_site[0],
        current_site.reshape(rows, phys * fwidth), current_block, penalty_weight,
    )
    return penalized, grown.transpose(1, 0, 2).reshape(1, w, bonds * w)


def solution(mesh):
    placed = (
        P("state", "bond", None),
        P("state", None, "bond", None),
        P("state", None, "bond", None),
        P("bond", None, "state"),
        P(None, "bond", "state"),
        P(),
    )
    return jax.shard_map(
        functools.partial(shards, mesh.shape["state"], mesh.shape["bond"]),
        mesh=mesh,
        in_specs=placed,
        out_specs=(P(None, "bond", "state"), P("state", "bond", None)),
        check_vma=False,
    )
```

```python
import functools

import jax
import jax.numpy as jnp
from jax import lax
from jax.experimental import pallas as pl
from jax.experimental.pallas import tpu as pltpu
from jax.sharding import PartitionSpec as P

MESH = pl.DeviceIdType.MESH
CORES = 2
TILE = 256


def kernel(
    states, bonds, rows_y,
    env_hbm, block_hbm, site_hbm, grow_hbm, current_hbm, weight_ref,
    pen_hbm, next_hbm,
    ebuf, abuf, stored, cbuf, psend, precv, mbuf, acc, pen, nsend, nrecv, iall,
    local_sem, out_sem, e_send, e_recv, a_send, a_recv, p_send, p_recv, m_send, m_recv,
    i_send, i_recv, n_send, n_recv, c_send, c_recv, line,
):
    nc, ny = CORES, rows_y
    nz = bonds // (nc * ny)
    rows, width = ebuf.shape[1:]
    pairs = block_hbm.shape[0]
    phys = site_hbm.shape[0]
    w = block_hbm.shape[1]
    per_group = TILE // rows
    per_row = ny * nc * rows // TILE
    groups = width // TILE
    gpp = groups // states
    fwidth = abuf.shape[2] // phys
    nfb = fwidth // w
    count = states * bonds

    k = lax.axis_index("state")
    me = lax.axis_index("bond")
    c = lax.rem(me, nc)
    y = lax.rem(lax.div(me, nc), ny)
    z = lax.div(me, nc * ny)
    flat = k * bonds + me

    def slot(zz, yy, cc):
        return (zz * ny + yy) * nc + cc

    e_load = pltpu.make_async_copy(env_hbm, ebuf.at[me], local_sem.at[0])
    a_load = pltpu.make_async_copy(grow_hbm, abuf.at[me], local_sem.at[1])
    e_load.start()
    c_loads = [
        pltpu.make_async_copy(
            current_hbm.at[:, :, pl.ds(g * TILE, TILE)], cbuf.at[k * gpp + g], local_sem.at[3]
        )
        for g in range(gpp)
    ]
    for copy in c_loads:
        copy.start()
    loads = []
    for q in range(pairs):
        loads.append(pltpu.make_async_copy(block_hbm.at[q], stored.at[pl.ds(q * w, w)], local_sem.at[2]))
    for s in range(phys):
        loads.append(
            pltpu.make_async_copy(site_hbm.at[s], stored.at[pl.ds((pairs + s) * w, w)], local_sem.at[2])
        )
    for copy in loads:
        copy.start()
    a_load.start()

    barrier = pltpu.get_barrier_semaphore()

    @pl.loop(1, count)
    def _(r):
        peer = lax.rem(flat + r, count)
        pl.semaphore_signal(
            barrier, inc=1, device_id=(lax.div(peer, bonds), lax.rem(peer, bonds)), device_id_type=MESH
        )

    pl.semaphore_wait(barrier, count - 1)

    env = (ebuf, e_send, e_recv)
    site = (abuf, a_send, a_recv)

    def copy_of(what, blk, dest):
        buf, ss, rs = what
        return pltpu.make_async_remote_copy(
            src_ref=buf.at[blk], dst_ref=buf.at[blk], send_sem=ss, recv_sem=rs.at[blk],
            device_id=(k, dest), device_id_type=MESH,
        )

    def act(what, blk, dest, drain):
        copy = copy_of(what, blk, dest)
        if drain:
            copy.wait_send()
        else:
            copy.start()

    def arrive(what, blk):
        copy_of(what, blk, me).wait_recv()

    detoured = ny == 2 and nz > 2

    def is_end(zz):
        return jnp.logical_or(zz == 0, zz == nz - 1)

    def spread(what, blk, drain, wide=True):
        @pl.when(jnp.logical_and(y > 0, wide))
        def _():
            act(what, blk, slot(z, y - 1, c), drain)

        @pl.when(jnp.logical_and(y < ny - 1, wide))
        def _():
            act(what, blk, slot(z, y + 1, c), drain)

        act(what, blk, slot(z, y, 1 - c), drain)

    def column(what, i, drain=False):
        if i == 0:
            blk = slot(z, y, c)

            @pl.when(z > 0)
            def _():
                act(what, blk, slot(z - 1, y, c), drain)

            @pl.when(z < nz - 1)
            def _():
                act(what, blk, slot(z + 1, y, c), drain)

            if not (detoured and what is site):
                spread(what, blk, drain)
            return
        for sign in (1, -1):
            zz = z - sign * i
            onward = z + sign

            @pl.when(jnp.logical_and(zz >= 0, zz < nz))
            def _():
                blk = slot(zz, y, c)
                if not drain:
                    arrive(what, blk)

                @pl.when(jnp.logical_and(onward >= 0, onward < nz))
                def _():
                    act(what, blk, slot(onward, y, c), drain)

                wide = jnp.logical_not(is_end(zz)) if detoured and what is site else True
                spread(what, blk, drain, wide)

    def detour(what, d, drain=False):
        if d == 0:
            blk = slot(z, 1 - y, c)
            if not drain:
                arrive(what, blk)

            @pl.when(z == 0)
            def _():
                act(what, blk, slot(1, y, c), drain)

            @pl.when(z == nz - 1)
            def _():
                act(what, blk, slot(nz - 2, y, c), drain)

            act(what, blk, slot(z, y, 1 - c), drain)
            return
        for sign, end in ((1, 0), (-1, nz - 1)):
            onward = z + sign

            @pl.when(z - sign * d == end)
            def _():
                blk = slot(end, 1 - y, c)
                if not drain:
                    arrive(what, blk)

                @pl.when(jnp.logical_and(onward >= 0, onward < nz))
                def _():
                    act(what, blk, slot(onward, y, c), drain)

                act(what, blk, slot(z, y, 1 - c), drain)

    def turn(j):
        least = jnp.minimum(z, nz - 1 - z)
        near = (j + 1) // 2
        inner = z - near if j % 2 else z + near
        far = j - least
        outer = jnp.where(z <= nz - 1 - z, z + far, z - far)
        return jnp.where(j <= 2 * least, inner, outer)

    def across(what, j, drain=False):
        if detoured and what is site and j == 0:
            return
        zz = turn(j)
        straight = jnp.logical_not(is_end(zz)) if detoured and what is site else True
        for u in range(1, ny):
            for sign in (1, -1):
                yy = y - sign * u
                onward = y + sign

                @pl.when(jnp.logical_and(jnp.logical_and(yy >= 0, yy < ny), straight))
                def _():
                    blk = slot(zz, yy, c)
                    if not drain:
                        arrive(what, blk)

                    @pl.when(jnp.logical_and(onward >= 0, onward < ny))
                    def _():
                        act(what, blk, slot(z, onward, c), drain)

                    act(what, blk, slot(z, y, 1 - c), drain)

    def sibling(what, j):
        zz = turn(j)
        for yy in range(ny):
            arrive(what, slot(zz, yy, 1 - c))

    def p_copy(g, peer):
        return pltpu.make_async_remote_copy(
            src_ref=psend.at[g], dst_ref=precv.at[k, lax.rem(g, gpp)], send_sem=p_send,
            recv_sem=p_recv.at[k], device_id=(peer, me), device_id_type=MESH,
        )

    def m_copy(g, peer):
        return pltpu.make_async_remote_copy(
            src_ref=mbuf.at[g, :, k], dst_ref=mbuf.at[g, :, k], send_sem=m_send,
            recv_sem=m_recv.at[k], device_id=(peer, me), device_id_type=MESH,
        )

    def c_copy(zz, peer):
        part = pl.ds(zz * per_row, per_row)
        return pltpu.make_async_remote_copy(
            src_ref=cbuf.at[part], dst_ref=cbuf.at[part], send_sem=c_send, recv_sem=c_recv.at[zz],
            device_id=(peer, me), device_id_type=MESH,
        )

    def share(drain=False):
        for j in range(nz):
            zz = turn(j)

            @pl.when(lax.div(zz * per_row, gpp) == k)
            def _():
                for other in range(1, states):
                    copy = c_copy(zz, lax.rem(k + other, states))
                    if drain:
                        copy.wait_send()
                    else:
                        copy.start()

    def project(j):
        zz = turn(j)

        @pl.when(lax.div(zz * per_row, gpp) != k)
        def _():
            c_copy(zz, k).wait_recv()

        @pl.loop(0, per_row)
        def _(r):
            g = zz * per_row + r
            left = ebuf[pl.ds(g * per_group, per_group)].reshape(TILE, width)
            prod = lax.dot_general(
                stored[...], left, (((1,), (1,)), ((), ())), preferred_element_type=jnp.float32
            )
            mbuf[g, :, k] = prod[pairs * w :].astype(jnp.bfloat16).reshape(phys, w, TILE)
            whole = prod[: pairs * w]
            here = cbuf[g].reshape(pairs * w, TILE).astype(jnp.float32)
            line[...] += jnp.sum((whole * here).reshape(pairs * w // 8, 8, TILE), axis=0)
            part = whole.astype(jnp.bfloat16)
            psend[g] = part
            owner = lax.div(g, gpp)

            @pl.when(owner == k)
            def _():
                precv[k, lax.rem(g, gpp)] = part

            for other in range(1, states):
                peer = lax.rem(k + other, states)

                m_copy(g, peer).start()

                @pl.when(owner == peer)
                def _():
                    p_copy(g, peer).start()

    def grow(j):
        zz = turn(j)

        @pl.loop(0, per_row)
        def _(r):
            g = zz * per_row + r
            right = abuf[pl.ds(g * per_group, per_group)].reshape(TILE, phys * fwidth)
            total = jnp.zeros((states * w, fwidth), jnp.float32)
            for s in range(phys):
                total = total + jnp.dot(
                    mbuf[g, s].reshape(states * w, TILE),
                    right[:, s * fwidth : (s + 1) * fwidth],
                    preferred_element_type=jnp.float32,
                )
            acc[...] += total

    def overlap():
        short = jnp.sum(line[...], axis=0, keepdims=True)
        total = short[:, :128]
        for at in range(128, TILE, 128):
            total = total + short[:, at : at + 128]
        iall[flat] = total

    def i_copy(peer):
        return pltpu.make_async_remote_copy(
            src_ref=iall.at[flat], dst_ref=iall.at[flat], send_sem=i_send, recv_sem=i_recv,
            device_id=(lax.div(peer, bonds), lax.rem(peer, bonds)), device_id_type=MESH,
        )

    def tell():
        @pl.loop(1, count)
        def _(r):
            i_copy(lax.rem(flat + r, count)).start()

    pen_copies = [
        pltpu.make_async_copy(pen.at[g], pen_hbm.at[:, :, pl.ds(g * TILE, TILE)], out_sem.at[0])
        for g in range(gpp)
    ]

    def penalize():
        rest = iall.at[pl.ds(0, count - 1)]
        pltpu.make_async_remote_copy(
            src_ref=rest, dst_ref=rest, send_sem=i_send, recv_sem=i_recv,
            device_id=(k, me), device_id_type=MESH,
        ).wait_recv()
        for other in range(1, states):
            peer = lax.rem(k + other, states)
            pltpu.make_async_remote_copy(
                src_ref=precv.at[peer], dst_ref=precv.at[peer], send_sem=p_send,
                recv_sem=p_recv.at[peer], device_id=(peer, me), device_id_type=MESH,
            ).wait_recv()
        scale = 1.0 / (phys * width)
        factors = [
            weight_ref[kk] * (jnp.sum(iall[kk * bonds : (kk + 1) * bonds]) * scale)
            for kk in range(states)
        ]
        for g in range(gpp):
            value = cbuf[k * gpp + g].reshape(pairs * w, TILE).astype(jnp.float32)
            for kk in range(states):
                value = value + factors[kk] * precv[kk, g].astype(jnp.float32)
            pen[g] = value.reshape(pairs, w, TILE)
            pen_copies[g].start()

    acc[...] = jnp.zeros_like(acc)
    line[...] = jnp.zeros_like(line)
    e_load.wait()
    for i in range(2 * nz):
        if i < nz:
            column(env, i)
        if i == 0:
            for copy in c_loads:
                copy.wait()
            share()
            if detoured:
                a_load.wait()
                spread(site, me, False)
        if i >= nz - 1 and i - (nz - 1) < nz:
            if i == nz - 1 and not detoured:
                a_load.wait()
            column(site, i - (nz - 1))
            if i == nz - 1 and detoured:
                detour(site, 0)
        if 1 <= i <= nz:
            across(env, i - 1)
            sibling(env, i - 1)
            if i == 1:
                for copy in loads:
                    copy.wait()
            project(i - 1)
            if i == nz:
                overlap()
                tell()
        if i >= nz:
            across(site, i - nz)
            if detoured and i > nz:
                detour(site, i - nz)
            sibling(site, i - nz)
            if i == nz:
                for other in range(1, states):
                    peer = lax.rem(k + other, states)
                    mine = mbuf.at[:, :, peer]
                    pltpu.make_async_remote_copy(
                        src_ref=mine, dst_ref=mine, send_sem=m_send, recv_sem=m_recv.at[peer],
                        device_id=(peer, me), device_id_type=MESH,
                    ).wait_recv()
            grow(i - nz)
            if i == min(nz + 1, 2 * nz - 1):
                penalize()

    def n_copy(kk, fb):
        return pltpu.make_async_remote_copy(
            src_ref=nsend.at[kk, fb], dst_ref=nrecv.at[me], send_sem=n_send, recv_sem=n_recv,
            device_id=(kk, k * nfb + fb), device_id_type=MESH,
        )

    def is_me(kk, fb):
        return jnp.logical_and(k == kk, me == k * nfb + fb)

    for kk in range(states):
        for fb in range(nfb):
            part = acc[kk * w : (kk + 1) * w, fb * w : (fb + 1) * w].T.astype(jnp.bfloat16)
            nsend[kk, fb] = part

            @pl.when(is_me(kk, fb))
            def _():
                nrecv[me] = part

            @pl.when(jnp.logical_not(is_me(kk, fb)))
            def _():
                n_copy(kk, fb).start()

    inside = lax.div(me, nfb) == k

    def all_of(number):
        rest = nrecv.at[pl.ds(0, number)]
        return pltpu.make_async_remote_copy(
            src_ref=rest, dst_ref=rest, send_sem=n_send, recv_sem=n_recv,
            device_id=(k, me), device_id_type=MESH,
        )

    for i in range(nz):
        for what in (env, site):
            column(what, i, drain=True)
            across(what, i, drain=True)
        if detoured:
            detour(site, i, drain=True)
            if i == 0:
                spread(site, me, True)

    share(drain=True)

    @pl.loop(0, groups)
    def _(g):
        for other in range(1, states):
            peer = lax.rem(k + other, states)

            @pl.when(lax.div(g, gpp) == peer)
            def _():
                p_copy(g, peer).wait_send()

            m_copy(g, peer).wait_send()

    @pl.loop(1, count)
    def _(r):
        i_copy(lax.rem(flat + r, count)).wait_send()

    for copy in pen_copies:
        copy.wait()
    for kk in range(states):
        for fb in range(nfb):
            @pl.when(jnp.logical_not(is_me(kk, fb)))
            def _():
                n_copy(kk, fb).wait_send()

    @pl.when(inside)
    def _():
        all_of(bonds - 1).wait_recv()

    @pl.when(jnp.logical_not(inside))
    def _():
        all_of(bonds).wait_recv()

    store = pltpu.make_async_copy(nrecv, next_hbm, out_sem.at[1])
    store.start()
    store.wait()


def shards(states, bonds, intersect_left, stored_block, stored_site, current_site, current_block, penalty_weight):
    rows, width = intersect_left.shape[1:]
    pairs, w = stored_block.shape[1:3]
    phys = stored_site.shape[1]
    fwidth = current_site.shape[2]
    groups = width // TILE
    gpp = groups // states
    rows_y = 1
    while 4 * rows_y * rows_y <= bonds // CORES:
        rows_y *= 2
    bf, f32 = jnp.bfloat16, jnp.float32
    anywhere = pl.BlockSpec(memory_space=pl.ANY)
    dma = pltpu.SemaphoreType.DMA
    penalized, grown = pl.pallas_call(
        functools.partial(kernel, states, bonds, rows_y),
        out_shape=(
            jax.ShapeDtypeStruct(current_block.shape, f32),
            jax.ShapeDtypeStruct((bonds, w, w), bf),
        ),
        in_specs=[anywhere] * 5 + [pl.BlockSpec(memory_space=pltpu.SMEM)],
        out_specs=(anywhere, anywhere),
        scratch_shapes=[
            pltpu.VMEM((bonds, rows, width), bf),
            pltpu.VMEM((bonds, rows, phys * fwidth), bf),
            pltpu.VMEM(((pairs + phys) * w, width), bf),
            pltpu.VMEM((groups, pairs, w, TILE), bf),
            pltpu.VMEM((groups, pairs * w, TILE), bf),
            pltpu.VMEM((states, gpp, pairs * w, TILE), bf),
            pltpu.VMEM((groups, phys, states, w, TILE), bf),
            pltpu.VMEM((states * w, fwidth), f32),
            pltpu.VMEM((gpp, pairs, w, TILE), f32),
            pltpu.VMEM((states, fwidth // w, w, w), bf),
            pltpu.VMEM((bonds, w, w), bf),
            pltpu.VMEM((states * bonds, 1, 128), f32),
            dma((4,)), dma((2,)),
            dma, dma((bonds,)), dma, dma((bonds,)),
            dma, dma((states,)), dma, dma((states,)),
            dma, dma, dma, dma,
            dma, dma((bonds,)),
            pltpu.VMEM((8, TILE), f32),
        ],
        compiler_params=pltpu.CompilerParams(
            collective_id=0, has_side_effects=True, vmem_limit_bytes=60 * 1024 * 1024
        ),
    )(
        intersect_left[0], stored_block[0], stored_site[0],
        current_site.reshape(rows, phys * fwidth), current_block, penalty_weight,
    )
    return penalized, grown.transpose(1, 0, 2).reshape(1, w, bonds * w)


def solution(mesh):
    placed = (
        P("state", "bond", None),
        P("state", None, "bond", None),
        P("state", None, "bond", None),
        P("bond", None, "state"),
        P(None, "bond", "state"),
        P(),
    )
    return jax.shard_map(
        functools.partial(shards, mesh.shape["state"], mesh.shape["bond"]),
        mesh=mesh,
        in_specs=placed,
        out_specs=(P(None, "bond", "state"), P("state", "bond", None)),
        check_vma=False,
    )
```
